32 devices in a mesh: expert: 16 (over z, y, x), dp: 2 (over core).
Axes of the slice: x: 2, y: 2, z: 4, core: 2. Of those that a mesh axis runs over, the one named last changes fastest.
Arguments:
- tokens: bfloat16 [8192, 4096], P('expert', 'dp'), may hold values from -6 to 6
- cotangent: bfloat16 [8192, 4096], P('expert', 'dp'), may hold values from -6 to 6
- routes: int32 [8192, 8], P('expert'), may hold values from 0 to 15, all different within a row; in each aligned block of 512 rows (0 to 511, 512 to 1023, ...) at most 512 rows name the same one
- probs: bfloat16 [8192, 8], P('expert'), may hold values from 0.099609375 to 1
- expert_slot: int32 [16], replicated, may hold values from 0 to 15, each once
- pull_flags: int32 [16], replicated, may hold values 0 or 1
- w_gate: bfloat16 [16, 768, 4096], P('expert', None, 'dp'), may hold values from -0.09375 to 0.09375
- w_up: bfloat16 [16, 768, 4096], P('expert', None, 'dp'), may hold values from -0.09375 to 0.09375
- w_down: bfloat16 [16, 768, 4096], P('expert', None, 'dp'), may hold values from -0.21875 to 0.21875
Outputs:
- expert_out: bfloat16 [8192, 4096], P('expert', 'dp')
- token_grad: bfloat16 [8192, 4096], P('expert', 'dp')
- gate_grad: bfloat16 [16, 768, 4096], P('expert', None, 'dp')
- up_grad: bfloat16 [16, 768, 4096], P('expert', None, 'dp')
- down_grad: bfloat16 [16, 768, 4096], P('expert', None, 'dp')
The draws below stay inside these ranges and needn't reach their ends.
Inputs may be any that keep to these rules, and one draw needn't show every extreme that they name: `routes`: each row names 8 different experts. Within the 512 rows of one token batch no expert is named by more than 512 rows, and in some batch some expert is named by exactly 512 rows. `expert_slot`: A permutation of the experts.
All inputs are finite; a program needn't handle non-finite values.
Results may differ from the reference program's by a relative error of at most 0.006.
Values may be sent and summed in bfloat16 or wider, within the bound.
No kernel may reach another device: no remote copies, remote signals or barrier semaphores. Data moves between devices by JAX's collectives and lax.ppermute only.
A program may use at most 128 MiB of HBM per device.

```python
import math
import jax
import jax.numpy as jnp
import numpy as np
from jax import lax

D = 4096
FF = 768
TOP = 8
TOK_DEV = 512
EXPERTS = 16
TOKENS = 8192
CAP = 512


def place_ends(values, stream_key, low, top_value):
    index_at = [jax.random.randint(jax.random.fold_in(stream_key, axis), (), 0, length) for axis, length in enumerate(values.shape)]
    widest = values.shape.index(max(values.shape))
    beside = index_at[:widest] + [(index_at[widest] + 1) % values.shape[widest]] + index_at[widest + 1:]
    return values.at[tuple(index_at)].set(low).at[tuple(beside)].set(top_value)


def steps_of(stream_key, shape, pieces, low, high):
    def one(dim, shards_of):
        draws = jax.random.uniform(jax.random.fold_in(jax.random.fold_in(stream_key, 6), dim), (shards_of,), jnp.float32, low / len(pieces), high / len(pieces))
        return jnp.repeat(jnp.exp(draws), shape[dim] // shards_of).reshape((-1,) + (1,) * (len(shape) - dim - 1))

    loudness = one(*pieces[0])
    for cut in pieces[1:]:
        loudness = loudness * one(*cut)
    return loudness


def shared_out(key, own, number, rows, count, top, most, lean):
    order = jax.random.permutation(key, count)
    crowded, common = portions_of(count, rows * top, most, lean, True), portions_of(count, rows * top, most, lean, False)
    places = jnp.arange(count)

    def named(lengths, turn):
        used = int((lengths > 0).sum())
        fixed = max(1, used // 4)
        passed = fixed + (places - fixed + turn * (used - fixed)) % max(1, count - fixed)
        return jnp.zeros((count,), jnp.int32).at[order[jnp.where(places < fixed, places, passed)]].set(jnp.asarray(lengths, jnp.int32))

    lengths = jnp.where(number % 4 == 0, named(crowded, number // 4), named(common, number - number // 4 - 1))
    mixed = jax.random.permutation(jax.random.fold_in(own, 3), count)
    source_of, taker = mixed[0:count // 2 * 2:2], mixed[1:count // 2 * 2:2]
    room = jnp.minimum(lengths[source_of] - 1, most - lengths[taker]) // 2
    room = jnp.where((source_of == order[0]) | (taker == order[0]) | (lengths[taker] == 0), 0, jnp.maximum(room, 0))
    passed = jax.random.randint(jax.random.fold_in(own, 4), (count // 2,), 0, 1 << 20) % (room + 1)
    lengths = lengths.at[source_of].add(-passed).at[taker].add(passed)
    members = jnp.searchsorted(jnp.cumsum(lengths), jnp.arange(rows * top), side="right").astype(jnp.int32)
    grid = members.reshape(top, rows).T
    grid = grid[jax.random.permutation(jax.random.fold_in(own, 1), rows)]
    turn = jax.random.randint(jax.random.fold_in(own, 2), (rows, 1), 0, top)
    return jnp.take_along_axis(grid, (jnp.arange(top)[None, :] + turn) % top, axis=1)


def portions_of(number_of, total, reach, lean, full):
    portions = [(1 << 20) // math.isqrt(standing ** lean) + 1 for standing in range(1, number_of + 1)]
    largest = reach if full else min(reach, max(-(-total // number_of), total * portions[0] // sum(portions)))
    least = 1 if total - largest >= number_of - 1 else 0
    counts, spare = [largest] + [least] * (number_of - 1), total - largest - least * (number_of - 1)
    while spare > 0:
        free = [i for i in range(1, number_of) if counts[i] < largest] or [i for i in range(1, number_of) if counts[i] < reach]
        pool, remaining = sum([portions[i] for i in free]), spare
        for i in free:
            more = min(reach - counts[i], max(1, remaining * portions[i] // pool), spare)
            counts[i] = counts[i] + more
            spare = spare - more
    return np.array(counts)


def gaussian(key, dims, deviation, most, shards=(), kind=jnp.bfloat16):
    values = deviation * jax.random.normal(key, dims, jnp.float32)
    if shards:
        values = values * steps_of(key, dims, shards, -0.22, 0.18)
    return jnp.clip(values, -most, most).astype(kind)


def setup_inputs(seed: int = 0) -> dict:
    splits = jax.random.split(jax.random.key(seed), 10)
    tokens = gaussian(splits[0], (TOKENS, D), 1.0, 6.0, ((0, 16), (1, 2)))
    cotangent = gaussian(splits[1], (TOKENS, D), 1.0, 6.0, ((0, 16), (1, 2)))
    routes_keys = jax.random.split(jax.random.fold_in(splits[2], 1), TOKENS // TOK_DEV)
    routes_turns = jax.random.permutation(jax.random.fold_in(splits[2], 3), TOKENS // TOK_DEV)
    routes = jax.vmap(lambda own, number: shared_out(jax.random.fold_in(splits[2], 2), own, number, TOK_DEV, EXPERTS, TOP, CAP, 2))(routes_keys, routes_turns).reshape((TOKENS, TOP))
    probs = jnp.clip(0.099609375 + 0.9003906 * jax.random.uniform(splits[3], (TOKENS, TOP), jnp.float32) ** steps_of(splits[3], (TOKENS, TOP), ((0, 16),), -0.2, 0.2), 0.099609375, 1.0).astype(jnp.bfloat16)
    expert_slot = jax.random.permutation(splits[4], EXPERTS).astype(jnp.int32)
    pull_flags = place_ends((jax.random.randint(splits[5], (EXPERTS,), 0, 4) < 3).astype(jnp.int32), jax.random.fold_in(splits[5], 1), 0, 1)
    w_gate = gaussian(splits[6], (EXPERTS, FF, D), D ** -0.5, 0.09375, ((0, 16), (2, 2)))
    w_up = gaussian(splits[7], (EXPERTS, FF, D), D ** -0.5, 0.09375, ((0, 16), (2, 2)))
    w_down = gaussian(splits[8], (EXPERTS, FF, D), FF ** -0.5, 0.21875, ((0, 16), (2, 2)))
    return dict(tokens=tokens, cotangent=cotangent, routes=routes, probs=probs, expert_slot=expert_slot, pull_flags=pull_flags, w_gate=w_gate, w_up=w_up, w_down=w_down)


def silu_parts(gate_val):
    sigmoid_val = jax.nn.sigmoid(gate_val)
    return gate_val * sigmoid_val, sigmoid_val * (1.0 + gate_val * (1.0 - sigmoid_val))


def slot_rows(route_ids, weights_in, expert, scale, capacity):
    count = route_ids.shape[0]
    hit = route_ids == expert
    member = jnp.any(hit, axis=1)
    weight = jnp.sum(jnp.where(hit, weights_in.astype(jnp.float32), 0.0), axis=1) * scale
    rank = jnp.cumsum(member.astype(jnp.int32), dtype=jnp.int32) - 1
    entries = jnp.arange(capacity, dtype=jnp.int32)
    chosen = member[None, :] & (rank[None, :] == entries[:, None])
    positions = jnp.arange(count, dtype=jnp.int32)
    index = jnp.sum(jnp.where(chosen, positions[None, :], 0), axis=1, dtype=jnp.int32)
    index = jnp.where(jnp.any(chosen, axis=1), index, count).astype(jnp.int32)
    return index, jnp.take(weight, index, mode="fill", fill_value=0.0)


def hidden_values(gate_val, up_val, back_val, rows_w):
    activated, slope_val = silu_parts(gate_val)
    weight_col = rows_w[..., None]
    scaled = (weight_col * activated * up_val).astype(jnp.bfloat16)
    grad_gate = (back_val * weight_col * up_val * slope_val).astype(jnp.bfloat16)
    grad_up = (back_val * weight_col * activated).astype(jnp.bfloat16)
    return scaled, grad_gate, grad_up


def column_pass(x_col, dy_col, routes_col, probs_col, expert, scale, wg, wu, wd):
    index, rows_w = slot_rows(routes_col, probs_col, expert, scale, CAP)
    rows_x = jnp.take(x_col, index, axis=0, mode="fill", fill_value=0)
    rows_dy = jnp.take(dy_col, index, axis=0, mode="fill", fill_value=0)
    gate_val = jnp.dot(rows_x, wg.T, preferred_element_type=jnp.float32)
    up_val = jnp.dot(rows_x, wu.T, preferred_element_type=jnp.float32)
    back_val = jnp.dot(rows_dy, wd.T, preferred_element_type=jnp.float32)
    scaled, grad_gate, grad_up = hidden_values(gate_val, up_val, back_val, rows_w)
    out_rows = jnp.dot(scaled, wd, preferred_element_type=jnp.float32)
    in_rows = jnp.dot(grad_gate, wg, preferred_element_type=jnp.float32)
    in_rows = in_rows + jnp.dot(grad_up, wu, preferred_element_type=jnp.float32)
    grad_terms = (jnp.dot(grad_gate.T, rows_x, preferred_element_type=jnp.float32),
                  jnp.dot(grad_up.T, rows_x, preferred_element_type=jnp.float32),
                  jnp.dot(scaled.T, rows_dy, preferred_element_type=jnp.float32))
    return index, out_rows, in_rows, grad_terms


def rounded(value):
    return lax.optimization_barrier(value.astype(jnp.bfloat16)).astype(jnp.float32)


def reference(tokens, cotangent, routes, probs, expert_slot, pull_flags, w_gate, w_up, w_down):
    labels = jnp.arange(EXPERTS, dtype=jnp.int32)
    experts_of = jnp.zeros((EXPERTS,), jnp.int32).at[expert_slot].set(labels)

    def column_slice(array, column):
        return lax.dynamic_slice_in_dim(array, column * TOK_DEV, TOK_DEV, 0)

    def pass_for(column, slot, scale):
        return column_pass(column_slice(tokens, column), column_slice(cotangent, column),
                           column_slice(routes, column), column_slice(probs, column),
                           experts_of[slot], scale, w_gate[slot], w_up[slot], w_down[slot])

    def outputs_of(column):
        following = (column + 1) % EXPERTS
        flag = pull_flags[column].astype(jnp.float32)
        out_rows = jnp.zeros((TOK_DEV, D), jnp.float32)
        in_rows = jnp.zeros((TOK_DEV, D), jnp.float32)
        for result in (pass_for(column, column, 1.0), pass_for(column, following, flag)):
            out_rows = out_rows.at[result[0]].add(result[1], mode="drop")
            in_rows = in_rows.at[result[0]].add(result[2], mode="drop")
        return out_rows.astype(jnp.bfloat16), in_rows.astype(jnp.bfloat16)

    expert_out, token_grad = lax.map(outputs_of, labels)

    def grads_of(slot):
        earlier = (slot - 1 + EXPERTS) % EXPERTS
        mine = pass_for(slot, slot, 1.0)[3]
        theirs = pass_for(earlier, slot, pull_flags[earlier].astype(jnp.float32))[3]
        return tuple((rounded(first) + rounded(second)).astype(jnp.bfloat16) for first, second in zip(mine, theirs))

    gate_grad, up_grad, down_grad = lax.map(grads_of, labels)
    return (expert_out.reshape(TOKENS, D), token_grad.reshape(TOKENS, D), gate_grad, up_grad, down_grad)
```

```python
import jax
import jax.numpy as jnp
from jax import lax
from jax.sharding import PartitionSpec as P


def passed_along(value, axis, steps):
    count = lax.axis_size(axis)
    pairs = [(source, (source + steps) % count) for source in range(count)]
    return lax.ppermute(value, axis, pairs)


def route_weight(route_ids, weights_in, expert):
    hit = route_ids == expert
    return jnp.sum(jnp.where(hit, weights_in.astype(jnp.float32), 0.0), axis=1)


def slot_rows(route_ids, expert, capacity):
    count = route_ids.shape[0]
    member = jnp.any(route_ids == expert, axis=1)
    rank = jnp.cumsum(member.astype(jnp.int32), dtype=jnp.int32) - 1
    entries = jnp.arange(capacity, dtype=jnp.int32)
    chosen = member[None, :] & (rank[None, :] == entries[:, None])
    positions = jnp.arange(count, dtype=jnp.int32)
    index = jnp.sum(jnp.where(chosen, positions[None, :], 0), axis=1, dtype=jnp.int32)
    return jnp.where(jnp.any(chosen, axis=1), index, count)


def take_rows(array, index):
    if index is None:
        return array
    return jnp.take(array, index, axis=0, mode="fill", fill_value=0)


def add_rows(own, own_index, far, far_index, count):
    if own_index is None:
        return own + far
    empty = jnp.zeros((count, own.shape[1]), jnp.float32)
    return empty.at[own_index].add(own, mode="drop").at[far_index].add(far, mode="drop")


def summed_over_dp(part):
    if lax.axis_size("dp") == 2:
        return part + passed_along(part, "dp", 1)
    part = lax.psum_scatter(part, "dp", scatter_dimension=1, tiled=True)
    return lax.all_gather(part, "dp", axis=1, tiled=True)


def rows_by_weights(rows, weight):
    return lax.dot_general(rows, weight, (((1,), (1,)), ((), ())), preferred_element_type=jnp.float32)


def hidden_by_weights(hidden, weight):
    return jnp.dot(hidden, weight, preferred_element_type=jnp.float32)


def over_rows(hidden, rows):
    term = lax.dot_general(hidden, rows, (((0,), (0,)), ((), ())), preferred_element_type=jnp.float32)
    return term.astype(jnp.bfloat16)


def act_of(gate_val, up_val, weight_col):
    return (weight_col * (gate_val * jax.nn.sigmoid(gate_val)) * up_val).astype(jnp.bfloat16)


def slopes_of(gate_val, up_val, back_val, weight_col):
    sigmoid_val = jax.nn.sigmoid(gate_val)
    weighted = back_val * weight_col
    grad_gate = weighted * up_val * (sigmoid_val * (1.0 + gate_val * (1.0 - sigmoid_val)))
    grad_up = weighted * (gate_val * sigmoid_val)
    return grad_gate.astype(jnp.bfloat16), grad_up.astype(jnp.bfloat16)


def per_device(tokens, cotangent, routes, probs, expert_slot, pull_flags, w_gate, w_up, w_down):
    columns = lax.axis_size("expert")
    column = lax.axis_index("expert")
    count = tokens.shape[0]
    capacity = min(count, count * routes.shape[1] * 2 // columns)
    labels = jnp.arange(columns, dtype=jnp.int32)
    following = (column + 1) % columns
    wg, wu, wd = w_gate[0], w_up[0], w_down[0]

    def owner_expert(slot):
        return jnp.sum(jnp.where(expert_slot == slot, labels, 0), dtype=jnp.int32)

    flag = pull_flags[column].astype(jnp.float32)
    own_expert, next_expert = owner_expert(column), owner_expert(following)
    own_weight = route_weight(routes, probs, own_expert)
    next_weight = route_weight(routes, probs, next_expert) * flag
    own_index = next_index = None
    if capacity < count:
        own_index = slot_rows(routes, own_expert, capacity)
        next_index = slot_rows(routes, next_expert, capacity)
        own_weight = jnp.take(own_weight, own_index, mode="fill", fill_value=0.0)
        next_weight = jnp.take(next_weight, next_index, mode="fill", fill_value=0.0)
    own_x, own_dy = take_rows(tokens, own_index), take_rows(cotangent, own_index)
    far_x = passed_along(take_rows(tokens, next_index), "expert", 1)
    far_w = passed_along(next_weight.astype(jnp.bfloat16), "expert", 1)
    far_dy = passed_along(take_rows(cotangent, next_index), "expert", 1)
    own_w, far_w = own_weight[:, None], far_w.astype(jnp.float32)[:, None]

    own_gate = rows_by_weights(own_x, wg)
    own_gate = summed_over_dp(own_gate)
    own_up = summed_over_dp(rows_by_weights(own_x, wu))
    own_back = summed_over_dp(rows_by_weights(own_dy, wd))
    own_act = act_of(own_gate, own_up, own_w)
    own_dgate, own_dup = slopes_of(own_gate, own_up, own_back, own_w)
    own_out = hidden_by_weights(own_act, wd)
    own_in = hidden_by_weights(own_dgate, wg) + hidden_by_weights(own_dup, wu)
    own_out, own_in = lax.optimization_barrier((own_out, own_in))
    own_grads = (over_rows(own_dgate, own_x), over_rows(own_dup, own_x), over_rows(own_act, own_dy))
    own_grads = lax.optimization_barrier(own_grads)

    far_gate = summed_over_dp(rows_by_weights(far_x, wg))
    far_up = summed_over_dp(rows_by_weights(far_x, wu))
    far_act = act_of(far_gate, far_up, far_w)
    far_out = hidden_by_weights(far_act, wd).astype(jnp.bfloat16)
    next_out = passed_along(far_out, "expert", -1)

    far_dy, far_out = lax.optimization_barrier((far_dy, far_out))
    far_back = rows_by_weights(far_dy, wd)
    far_back = summed_over_dp(far_back)
    far_dgate, far_dup = slopes_of(far_gate, far_up, far_back, far_w)
    far_in = hidden_by_weights(far_dgate, wg) + hidden_by_weights(far_dup, wu)
    next_in = passed_along(far_in.astype(jnp.bfloat16), "expert", -1)

    far_grads = (over_rows(far_dgate, far_x), over_rows(far_dup, far_x), over_rows(far_act, far_dy))
    grad_sums = [
        (mine.astype(jnp.float32) + theirs.astype(jnp.float32)).astype(jnp.bfloat16)[None]
        for mine, theirs in zip(own_grads, far_grads)
    ]
    out_rows = add_rows(own_out, own_index, next_out.astype(jnp.float32), next_index, count)
    in_rows = add_rows(own_in, own_index, next_in.astype(jnp.float32), next_index, count)
    return (out_rows.astype(jnp.bfloat16), in_rows.astype(jnp.bfloat16), *grad_sums)


def solution(mesh):
    return jax.shard_map(
        per_device,
        mesh=mesh,
        in_specs=(
            P("expert", "dp"),
            P("expert", "dp"),
            P("expert", None),
            P("expert", None),
            P(),
            P(),
            P("expert", None, "dp"),
            P("expert", None, "dp"),
            P("expert", None, "dp"),
        ),
        out_specs=(
            P("expert", "dp"),
            P("expert", "dp"),
            P("expert", None, "dp"),
            P("expert", None, "dp"),
            P("expert", None, "dp"),
        ),
        check_vma=False,
    )
```

```python
import jax
import jax.numpy as jnp
from jax import lax
from jax.sharding import PartitionSpec as P


def passed_along(value, axis, steps):
    count = lax.axis_size(axis)
    pairs = [(source, (source + steps) % count) for source in range(count)]
    return lax.ppermute(value, axis, pairs)


def route_weight(route_ids, weights_in, expert):
    hit = route_ids == expert
    return jnp.sum(jnp.where(hit, weights_in.astype(jnp.float32), 0.0), axis=1)


def slot_rows(route_ids, expert, capacity):
    count = route_ids.shape[0]
    member = jnp.any(route_ids == expert, axis=1)
    rank = jnp.cumsum(member.astype(jnp.int32), dtype=jnp.int32) - 1
    entries = jnp.arange(capacity, dtype=jnp.int32)
    chosen = member[None, :] & (rank[None, :] == entries[:, None])
    positions = jnp.arange(count, dtype=jnp.int32)
    index = jnp.sum(jnp.where(chosen, positions[None, :], 0), axis=1, dtype=jnp.int32)
    return jnp.where(jnp.any(chosen, axis=1), index, count)


def take_rows(array, index):
    if index is None:
        return array
    return jnp.take(array, index, axis=0, mode="fill", fill_value=0)


def add_rows(own, own_index, far, far_index, count):
    if own_index is None:
        return own + far
    empty = jnp.zeros((count, own.shape[1]), jnp.float32)
    return empty.at[own_index].add(own, mode="drop").at[far_index].add(far, mode="drop")


def summed_over_dp(part):
    if lax.axis_size("dp") == 2:
        return part + passed_along(part, "dp", 1)
    part = lax.psum_scatter(part, "dp", scatter_dimension=1, tiled=True)
    return lax.all_gather(part, "dp", axis=1, tiled=True)


def rows_by_weights(rows, weight):
    return lax.dot_general(rows, weight, (((1,), (1,)), ((), ())), preferred_element_type=jnp.float32)


def hidden_by_weights(hidden, weight):
    return jnp.dot(hidden, weight, preferred_element_type=jnp.float32)


def over_rows(hidden, rows):
    term = lax.dot_general(hidden, rows, (((0,), (0,)), ((), ())), preferred_element_type=jnp.float32)
    return term.astype(jnp.bfloat16)


def act_of(gate_val, up_val, weight_col):
    return (weight_col * (gate_val * jax.nn.sigmoid(gate_val)) * up_val).astype(jnp.bfloat16)


def slopes_of(gate_val, up_val, back_val, weight_col):
    sigmoid_val = jax.nn.sigmoid(gate_val)
    weighted = back_val * weight_col
    grad_gate = weighted * up_val * (sigmoid_val * (1.0 + gate_val * (1.0 - sigmoid_val)))
    grad_up = weighted * (gate_val * sigmoid_val)
    return grad_gate.astype(jnp.bfloat16), grad_up.astype(jnp.bfloat16)


def per_device(tokens, cotangent, routes, probs, expert_slot, pull_flags, w_gate, w_up, w_down):
    columns = lax.axis_size("expert")
    column = lax.axis_index("expert")
    count = tokens.shape[0]
    capacity = min(count, count * routes.shape[1] * 2 // columns)
    labels = jnp.arange(columns, dtype=jnp.int32)
    following = (column + 1) % columns
    wg, wu, wd = w_gate[0], w_up[0], w_down[0]

    def owner_expert(slot):
        return jnp.sum(jnp.where(expert_slot == slot, labels, 0), dtype=jnp.int32)

    flag = pull_flags[column].astype(jnp.float32)
    own_expert, next_expert = owner_expert(column), owner_expert(following)
    own_weight = route_weight(routes, probs, own_expert)
    next_weight = route_weight(routes, probs, next_expert) * flag
    own_index = next_index = None
    if capacity < count:
        own_index = slot_rows(routes, own_expert, capacity)
        next_index = slot_rows(routes, next_expert, capacity)
        own_weight = jnp.take(own_weight, own_index, mode="fill", fill_value=0.0)
        next_weight = jnp.take(next_weight, next_index, mode="fill", fill_value=0.0)
    own_x, own_dy = take_rows(tokens, own_index), take_rows(cotangent, own_index)
    far_x = passed_along(take_rows(tokens, next_index), "expert", 1)
    far_w = passed_along(next_weight.astype(jnp.bfloat16), "expert", 1)
    next_dy = take_rows(cotangent, next_index)
    dy_cut = capacity - capacity // 16
    cut = capacity - capacity // 8
    far_dy_head = passed_along(next_dy[:dy_cut], "expert", 1)
    far_dy_tail = passed_along(next_dy[dy_cut:], "expert", 1)
    own_w, far_w = own_weight[:, None], far_w.astype(jnp.float32)[:, None]

    own_gate = rows_by_weights(own_x, wg)
    own_gate = summed_over_dp(own_gate)
    own_up = summed_over_dp(rows_by_weights(own_x, wu))
    own_back = summed_over_dp(rows_by_weights(own_dy, wd))
    own_act = act_of(own_gate, own_up, own_w)
    own_dgate, own_dup = slopes_of(own_gate, own_up, own_back, own_w)
    own_out = hidden_by_weights(own_act, wd)
    own_in = hidden_by_weights(own_dgate, wg) + hidden_by_weights(own_dup, wu)
    own_out, own_in = lax.optimization_barrier((own_out, own_in))
    own_grads = (over_rows(own_dgate, own_x), over_rows(own_dup, own_x), over_rows(own_act, own_dy))
    own_grads = lax.optimization_barrier(own_grads)

    far_gate = summed_over_dp(rows_by_weights(far_x, wg))
    far_up = summed_over_dp(rows_by_weights(far_x, wu))
    far_act = act_of(far_gate, far_up, far_w)
    far_out = hidden_by_weights(far_act, wd).astype(jnp.bfloat16)
    next_out = passed_along(far_out, "expert", -1)

    far_dy_head, far_dy_tail, far_out = lax.optimization_barrier((far_dy_head, far_dy_tail, far_out))
    far_dy = jnp.concatenate([far_dy_head, far_dy_tail])
    far_back = rows_by_weights(far_dy, wd)
    far_back = summed_over_dp(far_back)
    far_dgate, far_dup = slopes_of(far_gate, far_up, far_back, far_w)
    far_in = hidden_by_weights(far_dgate, wg) + hidden_by_weights(far_dup, wu)
    far_in = far_in.astype(jnp.bfloat16)
    next_in_head = passed_along(far_in[:cut], "expert", -1)
    next_in_tail = passed_along(far_in[cut:], "expert", -1)

    far_grads = (over_rows(far_dgate, far_x), over_rows(far_dup, far_x), over_rows(far_act, far_dy))
    grad_sums = [
        (mine.astype(jnp.float32) + theirs.astype(jnp.float32)).astype(jnp.bfloat16)[None]
        for mine, theirs in zip(own_grads, far_grads)
    ]
    out_rows = add_rows(own_out, own_index, next_out.astype(jnp.float32), next_index, count)
    if next_index is None:
        head = own_in + jnp.pad(next_in_head, ((0, count - cut), (0, 0))).astype(jnp.float32)
        head = lax.optimization_barrier(head.astype(jnp.bfloat16))
        tail = (own_in[cut:] + next_in_tail.astype(jnp.float32)).astype(jnp.bfloat16)
        in_rows = lax.dynamic_update_slice(head, tail, (cut, 0))
    else:
        next_in = jnp.concatenate([next_in_head, next_in_tail]).astype(jnp.float32)
        in_rows = add_rows(own_in, own_index, next_in, next_index, count).astype(jnp.bfloat16)
    return (out_rows.astype(jnp.bfloat16), in_rows, *grad_sums)


def solution(mesh):
    return jax.shard_map(
        per_device,
        mesh=mesh,
        in_specs=(
            P("expert", "dp"),
            P("expert", "dp"),
            P("expert", None),
            P("expert", None),
            P(),
            P(),
            P("expert", None, "dp"),
            P("expert", None, "dp"),
            P("expert", None, "dp"),
        ),
        out_specs=(
            P("expert", "dp"),
            P("expert", "dp"),
            P("expert", None, "dp"),
            P("expert", None, "dp"),
            P("expert", None, "dp"),
        ),
        check_vma=False,
    )
```

```python
import jax
import jax.numpy as jnp
from jax import lax
from jax.sharding import PartitionSpec as P


def passed_along(value, axis, steps):
    count = lax.axis_size(axis)
    pairs = [(source, (source + steps) % count) for source in range(count)]
    return lax.ppermute(value, axis, pairs)


def edge_pairs(count):
    return [(source, source + 1) for source in range(count - 1)], [(count - 1, 0)]


def route_weight(route_ids, weights_in, expert):
    hit = route_ids == expert
    return jnp.sum(jnp.where(hit, weights_in.astype(jnp.float32), 0.0), axis=1)


def slot_rows(route_ids, expert, capacity):
    count = route_ids.shape[0]
    member = jnp.any(route_ids == expert, axis=1)
    rank = jnp.cumsum(member.astype(jnp.int32), dtype=jnp.int32) - 1
    entries = jnp.arange(capacity, dtype=jnp.int32)
    chosen = member[None, :] & (rank[None, :] == entries[:, None])
    positions = jnp.arange(count, dtype=jnp.int32)
    index = jnp.sum(jnp.where(chosen, positions[None, :], 0), axis=1, dtype=jnp.int32)
    return jnp.where(jnp.any(chosen, axis=1), index, count)


def take_rows(array, index):
    if index is None:
        return array
    return jnp.take(array, index, axis=0, mode="fill", fill_value=0)


def add_rows(own, own_index, far, far_index, count):
    if own_index is None:
        return own + far
    empty = jnp.zeros((count, own.shape[1]), jnp.float32)
    return empty.at[own_index].add(own, mode="drop").at[far_index].add(far, mode="drop")


def summed_over_dp(part):
    if lax.axis_size("dp") == 2:
        return part + passed_along(part, "dp", 1)
    part = lax.psum_scatter(part, "dp", scatter_dimension=1, tiled=True)
    return lax.all_gather(part, "dp", axis=1, tiled=True)


def rows_by_weights(rows, weight):
    return lax.dot_general(rows, weight, (((1,), (1,)), ((), ())), preferred_element_type=jnp.float32)


def hidden_by_weights(hidden, weight):
    return jnp.dot(hidden, weight, preferred_element_type=jnp.float32)


def over_rows(hidden, rows):
    term = lax.dot_general(hidden, rows, (((0,), (0,)), ((), ())), preferred_element_type=jnp.float32)
    return term.astype(jnp.bfloat16)


def act_of(gate_val, up_val, weight_col):
    return (weight_col * (gate_val * jax.nn.sigmoid(gate_val)) * up_val).astype(jnp.bfloat16)


def slopes_of(gate_val, up_val, back_val, weight_col):
    sigmoid_val = jax.nn.sigmoid(gate_val)
    weighted = back_val * weight_col
    grad_gate = weighted * up_val * (sigmoid_val * (1.0 + gate_val * (1.0 - sigmoid_val)))
    grad_up = weighted * (gate_val * sigmoid_val)
    return grad_gate.astype(jnp.bfloat16), grad_up.astype(jnp.bfloat16)


def per_device(tokens, cotangent, routes, probs, expert_slot, pull_flags, w_gate, w_up, w_down):
    columns = lax.axis_size("expert")
    column = lax.axis_index("expert")
    count = tokens.shape[0]
    capacity = min(count, count * routes.shape[1] * 2 // columns)
    labels = jnp.arange(columns, dtype=jnp.int32)
    following = (column + 1) % columns
    wg, wu, wd = w_gate[0], w_up[0], w_down[0]

    def owner_expert(slot):
        return jnp.sum(jnp.where(expert_slot == slot, labels, 0), dtype=jnp.int32)

    flag = pull_flags[column].astype(jnp.float32)
    own_expert, next_expert = owner_expert(column), owner_expert(following)
    own_weight = route_weight(routes, probs, own_expert)
    next_weight = route_weight(routes, probs, next_expert) * flag
    own_index = next_index = None
    if capacity < count:
        own_index = slot_rows(routes, own_expert, capacity)
        next_index = slot_rows(routes, next_expert, capacity)
        own_weight = jnp.take(own_weight, own_index, mode="fill", fill_value=0.0)
        next_weight = jnp.take(next_weight, next_index, mode="fill", fill_value=0.0)
    own_x, own_dy = take_rows(tokens, own_index), take_rows(cotangent, own_index)
    far_x = passed_along(take_rows(tokens, next_index), "expert", 1)
    far_w = passed_along(next_weight.astype(jnp.bfloat16), "expert", 1)
    next_dy = take_rows(cotangent, next_index)
    dy_cut = capacity - capacity // 16
    cut = capacity - capacity // 8
    gate_cut = dy_cut - capacity // 32
    far_dy_head = passed_along(next_dy[:gate_cut], "expert", 1)
    near, wrapped = edge_pairs(columns)
    dy_near = lax.ppermute(next_dy[gate_cut:dy_cut], "expert", near)
    dy_wrapped = lax.ppermute(next_dy[gate_cut:dy_cut], "expert", wrapped)
    far_dy_tail = passed_along(next_dy[dy_cut:], "expert", 1)
    own_w, far_w = own_weight[:, None], far_w.astype(jnp.float32)[:, None]

    own_gate = rows_by_weights(own_x, wg)
    own_gate = summed_over_dp(own_gate)
    own_up = summed_over_dp(rows_by_weights(own_x, wu))
    own_back = summed_over_dp(rows_by_weights(own_dy, wd))
    own_act = act_of(own_gate, own_up, own_w)
    own_dgate, own_dup = slopes_of(own_gate, own_up, own_back, own_w)
    own_out = hidden_by_weights(own_act, wd)
    own_in = hidden_by_weights(own_dgate, wg) + hidden_by_weights(own_dup, wu)
    own_out, own_in = lax.optimization_barrier((own_out, own_in))
    own_grads = (over_rows(own_dgate, own_x), over_rows(own_dup, own_x), over_rows(own_act, own_dy))
    own_grads = lax.optimization_barrier(own_grads)

    far_gate = summed_over_dp(rows_by_weights(far_x, wg))
    far_up = summed_over_dp(rows_by_weights(far_x, wu))
    far_act = act_of(far_gate, far_up, far_w)
    far_out = hidden_by_weights(far_act, wd).astype(jnp.bfloat16)
    next_out = passed_along(far_out, "expert", -1)

    far_dy_head, dy_near, dy_wrapped, far_dy_tail, far_out = lax.optimization_barrier(
        (far_dy_head, dy_near, dy_wrapped, far_dy_tail, far_out)
    )
    dy_gate = jnp.where(column == 0, dy_wrapped, dy_near)
    far_dy = jnp.concatenate([far_dy_head, dy_gate, far_dy_tail])
    far_back = rows_by_weights(far_dy, wd)
    far_back = summed_over_dp(far_back)
    far_dgate, far_dup = slopes_of(far_gate, far_up, far_back, far_w)
    far_in = hidden_by_weights(far_dgate, wg) + hidden_by_weights(far_dup, wu)
    far_in = far_in.astype(jnp.bfloat16)
    next_in_head = passed_along(far_in[:cut], "expert", -1)
    next_in_tail = passed_along(far_in[cut:], "expert", -1)

    far_grads = (over_rows(far_dgate, far_x), over_rows(far_dup, far_x), over_rows(far_act, far_dy))
    grad_sums = [
        (mine.astype(jnp.float32) + theirs.astype(jnp.float32)).astype(jnp.bfloat16)[None]
        for mine, theirs in zip(own_grads, far_grads)
    ]
    out_rows = add_rows(own_out, own_index, next_out.astype(jnp.float32), next_index, count)
    if next_index is None:
        head = own_in + jnp.pad(next_in_head, ((0, count - cut), (0, 0))).astype(jnp.float32)
        head = lax.optimization_barrier(head.astype(jnp.bfloat16))
        tail = (own_in[cut:] + next_in_tail.astype(jnp.float32)).astype(jnp.bfloat16)
        in_rows = lax.dynamic_update_slice(head, tail, (cut, 0))
    else:
        next_in = jnp.concatenate([next_in_head, next_in_tail]).astype(jnp.float32)
        in_rows = add_rows(own_in, own_index, next_in, next_index, count).astype(jnp.bfloat16)
    return (out_rows.astype(jnp.bfloat16), in_rows, *grad_sums)


def solution(mesh):
    return jax.shard_map(
        per_device,
        mesh=mesh,
        in_specs=(
            P("expert", "dp"),
            P("expert", "dp"),
            P("expert", None),
            P("expert", None),
            P(),
            P(),
            P("expert", None, "dp"),
            P("expert", None, "dp"),
            P("expert", None, "dp"),
        ),
        out_specs=(
            P("expert", "dp"),
            P("expert", "dp"),
            P("expert", None, "dp"),
            P("expert", None, "dp"),
            P("expert", None, "dp"),
        ),
        check_vma=False,
    )
```

```python
import jax
import jax.numpy as jnp
from jax import lax
from jax.sharding import PartitionSpec as P


def passed_along(value, axis, steps):
    count = lax.axis_size(axis)
    pairs = [(source, (source + steps) % count) for source in range(count)]
    return lax.ppermute(value, axis, pairs)


def edge_pairs(count):
    return [(source, source + 1) for source in range(count - 1)], [(count - 1, 0)]


def route_weight(route_ids, weights_in, expert):
    hit = route_ids == expert
    return jnp.sum(jnp.where(hit, weights_in.astype(jnp.float32), 0.0), axis=1)


def slot_rows(route_ids, expert, capacity):
    count = route_ids.shape[0]
    member = jnp.any(route_ids == expert, axis=1)
    rank = jnp.cumsum(member.astype(jnp.int32), dtype=jnp.int32) - 1
    entries = jnp.arange(capacity, dtype=jnp.int32)
    chosen = member[None, :] & (rank[None, :] == entries[:, None])
    positions = jnp.arange(count, dtype=jnp.int32)
    index = jnp.sum(jnp.where(chosen, positions[None, :], 0), axis=1, dtype=jnp.int32)
    return jnp.where(jnp.any(chosen, axis=1), index, count)


def take_rows(array, index):
    if index is None:
        return array
    return jnp.take(array, index, axis=0, mode="fill", fill_value=0)


def add_rows(own, own_index, far, far_index, count):
    if own_index is None:
        return own + far
    empty = jnp.zeros((count, own.shape[1]), jnp.float32)
    return empty.at[own_index].add(own, mode="drop").at[far_index].add(far, mode="drop")


def summed_over_dp(part):
    if lax.axis_size("dp") == 2:
        return part + passed_along(part, "dp", 1)
    part = lax.psum_scatter(part, "dp", scatter_dimension=1, tiled=True)
    return lax.all_gather(part, "dp", axis=1, tiled=True)


def rows_by_weights(rows, weight):
    return lax.dot_general(rows, weight, (((1,), (1,)), ((), ())), preferred_element_type=jnp.float32)


def hidden_by_weights(hidden, weight):
    return jnp.dot(hidden, weight, preferred_element_type=jnp.float32)


def over_rows(hidden, rows):
    term = lax.dot_general(hidden, rows, (((0,), (0,)), ((), ())), preferred_element_type=jnp.float32)
    return term.astype(jnp.bfloat16)


def act_of(gate_val, up_val, weight_col):
    return (weight_col * (gate_val * jax.nn.sigmoid(gate_val)) * up_val).astype(jnp.bfloat16)


def slopes_of(gate_val, up_val, back_val, weight_col):
    sigmoid_val = jax.nn.sigmoid(gate_val)
    weighted = back_val * weight_col
    grad_gate = weighted * up_val * (sigmoid_val * (1.0 + gate_val * (1.0 - sigmoid_val)))
    grad_up = weighted * (gate_val * sigmoid_val)
    return grad_gate.astype(jnp.bfloat16), grad_up.astype(jnp.bfloat16)


def per_device(tokens, cotangent, routes, probs, expert_slot, pull_flags, w_gate, w_up, w_down):
    columns = lax.axis_size("expert")
    column = lax.axis_index("expert")
    count = tokens.shape[0]
    capacity = min(count, count * routes.shape[1] * 2 // columns)
    labels = jnp.arange(columns, dtype=jnp.int32)
    following = (column + 1) % columns
    wg, wu, wd = w_gate[0], w_up[0], w_down[0]

    def owner_expert(slot):
        return jnp.sum(jnp.where(expert_slot == slot, labels, 0), dtype=jnp.int32)

    flag = pull_flags[column].astype(jnp.float32)
    own_expert, next_expert = owner_expert(column), owner_expert(following)
    own_weight = route_weight(routes, probs, own_expert)
    next_weight = route_weight(routes, probs, next_expert) * flag
    own_index = next_index = None
    if capacity < count:
        own_index = slot_rows(routes, own_expert, capacity)
        next_index = slot_rows(routes, next_expert, capacity)
        own_weight = jnp.take(own_weight, own_index, mode="fill", fill_value=0.0)
        next_weight = jnp.take(next_weight, next_index, mode="fill", fill_value=0.0)
    own_x, own_dy = take_rows(tokens, own_index), take_rows(cotangent, own_index)
    far_x = passed_along(take_rows(tokens, next_index), "expert", 1)
    far_w = passed_along(next_weight.astype(jnp.bfloat16), "expert", 1)
    next_dy = take_rows(cotangent, next_index)
    dy_cut = capacity - 5 * capacity // 64
    cut = capacity - 8 * capacity // 64
    gate_cut = dy_cut - 2 * capacity // 64
    far_dy_head = passed_along(next_dy[:gate_cut], "expert", 1)
    near, wrapped = edge_pairs(columns)
    dy_near = lax.ppermute(next_dy[gate_cut:dy_cut], "expert", near)
    dy_wrapped = lax.ppermute(next_dy[gate_cut:dy_cut], "expert", wrapped)
    far_dy_tail = passed_along(next_dy[dy_cut:], "expert", 1)
    own_w, far_w = own_weight[:, None], far_w.astype(jnp.float32)[:, None]

    own_gate = rows_by_weights(own_x, wg)
    own_gate = summed_over_dp(own_gate)
    own_up = summed_over_dp(rows_by_weights(own_x, wu))
    own_back = summed_over_dp(rows_by_weights(own_dy, wd))
    own_act = act_of(own_gate, own_up, own_w)
    own_dgate, own_dup = slopes_of(own_gate, own_up, own_back, own_w)
    own_out = hidden_by_weights(own_act, wd)
    own_in = hidden_by_weights(own_dgate, wg) + hidden_by_weights(own_dup, wu)
    own_out, own_in = lax.optimization_barrier((own_out, own_in))
    own_grads = (over_rows(own_dgate, own_x), over_rows(own_dup, own_x), over_rows(own_act, own_dy))
    own_grads = lax.optimization_barrier(own_grads)

    far_gate = summed_over_dp(rows_by_weights(far_x, wg))
    far_up = summed_over_dp(rows_by_weights(far_x, wu))
    far_act = act_of(far_gate, far_up, far_w)
    far_out = hidden_by_weights(far_act, wd).astype(jnp.bfloat16)
    next_out = passed_along(far_out, "expert", -1)

    far_dy_head, dy_near, dy_wrapped, far_dy_tail, far_out = lax.optimization_barrier(
        (far_dy_head, dy_near, dy_wrapped, far_dy_tail, far_out)
    )
    dy_gate = jnp.where(column == 0, dy_wrapped, dy_near)
    far_dy = jnp.concatenate([far_dy_head, dy_gate, far_dy_tail])
    far_back = rows_by_weights(far_dy, wd)
    far_back = summed_over_dp(far_back)
    far_dgate, far_dup = slopes_of(far_gate, far_up, far_back, far_w)
    far_in = hidden_by_weights(far_dgate, wg) + hidden_by_weights(far_dup, wu)
    far_in = far_in.astype(jnp.bfloat16)
    next_in_head = passed_along(far_in[:cut], "expert", -1)
    next_in_tail = passed_along(far_in[cut:], "expert", -1)

    far_grads = (over_rows(far_dgate, far_x), over_rows(far_dup, far_x), over_rows(far_act, far_dy))
    grad_sums = [
        (mine.astype(jnp.float32) + theirs.astype(jnp.float32)).astype(jnp.bfloat16)[None]
        for mine, theirs in zip(own_grads, far_grads)
    ]
    out_rows = add_rows(own_out, own_index, next_out.astype(jnp.float32), next_index, count)
    if next_index is None:
        head = own_in + jnp.pad(next_in_head, ((0, count - cut), (0, 0))).astype(jnp.float32)
        head = lax.optimization_barrier(head.astype(jnp.bfloat16))
        tail = (own_in[cut:] + next_in_tail.astype(jnp.float32)).astype(jnp.bfloat16)
        in_rows = lax.dynamic_update_slice(head, tail, (cut, 0))
    else:
        next_in = jnp.concatenate([next_in_head, next_in_tail]).astype(jnp.float32)
        in_rows = add_rows(own_in, own_index, next_in, next_index, count).astype(jnp.bfloat16)
    return (out_rows.astype(jnp.bfloat16), in_rows, *grad_sums)


def solution(mesh):
    return jax.shard_map(
        per_device,
        mesh=mesh,
        in_specs=(
            P("expert", "dp"),
            P("expert", "dp"),
            P("expert", None),
            P("expert", None),
            P(),
            P(),
            P("expert", None, "dp"),
            P("expert", None, "dp"),
            P("expert", None, "dp"),
        ),
        out_specs=(
            P("expert", "dp"),
            P("expert", "dp"),
            P("expert", None, "dp"),
            P("expert", None, "dp"),
            P("expert", None, "dp"),
        ),
        check_vma=False,
    )
```
